512 devices in a mesh: seq: 64 (over x, y, core), dp: 8 (over z).
Axes of the slice: x: 4, y: 8, z: 8, core: 2. Of those that a mesh axis runs over, the one named last changes fastest.
Arguments:
- glu_input: bfloat16 [8, 49152, 1024], P('dp', 'seq'), may hold values from -2500 to 2500
- out_grad: bfloat16 [8, 49152, 1024], P('dp', 'seq'), may hold values from -50 to 50
- lengths: int32 [8], replicated, may hold values from 24576 to 49152, as said below
- depth_weight: float32 [512, 31], replicated, may hold values from -1.5 to 1.5
- bn_gain: float32 [512], replicated, may hold values from 0.5 to 2
- bn_shift: float32 [512], replicated, may hold values from -1 to 1
- proj_weight: bfloat16 [512, 1024], P('seq', 'dp'), may hold values from -0.25 to 0.25
Outputs:
- input_grad: bfloat16 [8, 49152, 1024], P('dp', 'seq')
- proj_grad: float32 [512, 1024], P('seq', 'dp')
- depth_grad: float32 [512, 31], P('seq')
- gain_grad: float32 [512], P('seq')
- shift_grad: float32 [512], P('seq')
The draws below stay inside these ranges and needn't reach their ends.
Inputs may be any that keep to these rules, and one draw needn't show every extreme that they name: `lengths`: at least one utterance has all 49152 frames valid.
All inputs are finite; a program needn't handle non-finite values.
Results may differ from the reference program's by a relative error of at most 0.0061.
Values may be sent and summed in bfloat16 or wider, within the bound.
No kernel may reach another device: no remote copies, remote signals or barrier semaphores. Data moves between devices by JAX's collectives and lax.ppermute only.
A program may use at most 64 MiB of HBM per device.

```python
import math
import jax
import jax.numpy as jnp
from jax import lax

C = 512
D = 1024
KERNEL = 31
HALF = 15
LENGTH = 49152
UTTS = 8


def draw_glu_input(key, part):
    keys = jax.random.split(jax.random.fold_in(key, 17), 5)
    shape = (UTTS, LENGTH, 2 * C)
    frames = jnp.arange(LENGTH, dtype=jnp.float32) / LENGTH
    noise = jnp.clip(jax.random.normal(keys[0], shape, jnp.float32), -4.0, 4.0)
    offsets = jax.random.uniform(keys[1], (2 * C,), jnp.float32, -1.5, 1.5)
    ramp_up = 1.0 + 2.0 * frames
    value_scale = jnp.exp(jax.random.uniform(keys[2], (C,), jnp.float32, 0.0, math.log(10.0)))
    gate_scale = 0.3 * jnp.exp(jax.random.uniform(keys[3], (C,), jnp.float32, 0.0, math.log(2.0)))
    columns = jnp.concatenate([value_scale, gate_scale])
    rough = jnp.exp(jax.random.uniform(keys[4], (UTTS, LENGTH, 1), jnp.float32, 0.0, math.log(4.0)))
    return ((offsets + noise) * columns * rough * ramp_up[None, :, None]).astype(jnp.bfloat16)


def draw_out_grad(key, part):
    keys = jax.random.split(jax.random.fold_in(key, 29), 2)
    shape = (UTTS, LENGTH, D)
    frames = jnp.arange(LENGTH, dtype=jnp.float32) / LENGTH
    rough = jnp.exp(jax.random.uniform(keys[1], (UTTS, LENGTH, 1), jnp.float32, 0.0, math.log(3.0)))
    ramp_up = 1.0 + 2.0 * frames
    noise = jnp.clip(jax.random.normal(keys[0], shape, jnp.float32), -4.0, 4.0)
    return (noise * rough * ramp_up[None, :, None]).astype(jnp.bfloat16)


def draw_lengths(key, part):
    keys = jax.random.split(jax.random.fold_in(key, 41), 2)
    base = jax.random.randint(keys[0], (UTTS,), LENGTH // 2, LENGTH + 1, dtype=jnp.int32)
    chosen = jax.random.randint(keys[1], (), 0, UTTS, dtype=jnp.int32)
    return jnp.where(jnp.arange(UTTS, dtype=jnp.int32) == chosen, jnp.int32(LENGTH), base).astype(jnp.int32)


def steps_of(own_key, shape, shards, smallest, top_value):
    level = 1.0
    for dim, blocks in shards:
        draws = jax.random.uniform(jax.random.fold_in(jax.random.fold_in(own_key, 6), dim), (blocks,), jnp.float32, smallest / len(shards), top_value / len(shards))
        level = level * jnp.repeat(jnp.exp(draws), shape[dim] // blocks).reshape((-1,) + (1,) * (len(shape) - 1 - dim))
    return level


def scatter_about(key, extent, scale, bound, pieces=(), held_as=jnp.bfloat16):
    result = scale * jax.random.normal(key, extent, jnp.float32)
    if pieces:
        result = result * steps_of(key, extent, pieces, -0.22, 0.18)
    return jnp.clip(result, -bound, bound).astype(held_as)


def setup_inputs(seed: int = 0) -> dict:
    key_of = jax.random.split(jax.random.key(seed), 8)
    return {
        "glu_input": draw_glu_input(jax.random.fold_in(key_of[7], 71), 0),
        "out_grad": draw_out_grad(jax.random.fold_in(key_of[7], 71), 0),
        "lengths": draw_lengths(jax.random.fold_in(key_of[7], 71), 0),
        "depth_weight": scatter_about(key_of[3], (C, KERNEL), 0.25, 1.5, (), jnp.float32),
        "bn_gain": jnp.clip(jax.random.uniform(key_of[4], (C,), jnp.float32, 0.5, 2.0), 0.5, 2.0),
        "bn_shift": jnp.clip(jax.random.uniform(key_of[5], (C,), jnp.float32, -1.0, 1.0), -1.0, 1.0),
        "proj_weight": scatter_about(key_of[6], (C, D), C ** -0.5, 0.25, ((0, 64), (1, 8))),
    }


EPSILON = 1e-05

def recompute(glu_row, length, depth_weight):
    frames = jnp.arange(LENGTH, dtype=jnp.int32)
    frame_mask = (frames < length).astype(jnp.float32)[:, None]
    values = glu_row[:, :C].astype(jnp.float32)
    gate_sigmoid = jax.nn.sigmoid(glu_row[:, C:].astype(jnp.float32))
    glu_out = (values * gate_sigmoid * frame_mask).astype(jnp.bfloat16)
    padded = jnp.pad(glu_out, ((HALF, HALF), (0, 0))).astype(jnp.float32)
    conv_out = jnp.zeros((LENGTH, C), jnp.float32)
    for offset in range(KERNEL):
        conv_out = conv_out + depth_weight[:, offset] * padded[offset:offset + LENGTH]
    return (frame_mask, values, gate_sigmoid, padded, conv_out)

def reference(glu_input, out_grad, lengths, depth_weight, bn_gain, bn_shift, proj_weight):
    frame_count = jnp.sum(lengths).astype(jnp.float32)
    grad_scale = float(UTTS * LENGTH) ** (-0.5)

    def conv_sums(utterance):
        frame_mask, _, _, _, conv_out = recompute(utterance[0], utterance[1], depth_weight)
        return lax.optimization_barrier(jnp.sum(frame_mask * conv_out, axis=0))
    mean_val = lax.optimization_barrier(jnp.sum(lax.map(conv_sums, (glu_input, lengths)), axis=0)) / frame_count

    def conv_squares(utterance):
        frame_mask, _, _, _, conv_out = recompute(utterance[0], utterance[1], depth_weight)
        return lax.optimization_barrier(jnp.sum(frame_mask * jnp.square(conv_out - mean_val), axis=0))
    variance = lax.optimization_barrier(jnp.sum(lax.map(conv_squares, (glu_input, lengths)), axis=0)) / frame_count
    inv_std = lax.rsqrt(variance + EPSILON)

    def backward_act(utterance):
        glu_row, grad_row, length = utterance
        frame_mask, values, gate_sigmoid, padded, conv_out = recompute(glu_row, length, depth_weight)
        normed = (conv_out - mean_val) * inv_std
        pre_act = bn_gain * normed + bn_shift
        pre_sig = jax.nn.sigmoid(pre_act)
        act_out = (frame_mask * pre_act * pre_sig).astype(jnp.bfloat16)
        act_grad = frame_mask * jnp.dot(grad_row, proj_weight.T, preferred_element_type=jnp.float32)
        pre_grad = act_grad * pre_sig * (1.0 + pre_act * (1.0 - pre_sig))
        return (frame_mask, values, gate_sigmoid, padded, normed, act_out, pre_grad)

    def second(utterance):
        _, _, _, _, normed, act_out, pre_grad = backward_act(utterance)
        weight_part = jnp.dot(act_out.T, utterance[1], preferred_element_type=jnp.float32)
        return (weight_part, lax.optimization_barrier(jnp.sum(pre_grad * normed, axis=0)), lax.optimization_barrier(jnp.sum(pre_grad, axis=0)))
    weight_parts, gain_parts, shift_parts = lax.map(second, (glu_input, out_grad, lengths))
    proj_grad = grad_scale * lax.optimization_barrier(jnp.sum(weight_parts, axis=0))
    gain_sum = lax.optimization_barrier(jnp.sum(gain_parts, axis=0))
    shift_sum = lax.optimization_barrier(jnp.sum(shift_parts, axis=0))

    def third(utterance):
        frame_mask, values, gate_sigmoid, padded, normed, _, pre_grad = backward_act(utterance)
        conv_grad = (frame_mask * inv_std * bn_gain * (pre_grad - shift_sum / frame_count - normed * gain_sum / frame_count)).astype(jnp.bfloat16)
        conv_wide = conv_grad.astype(jnp.float32)
        depth_part = jnp.stack([lax.optimization_barrier(jnp.sum(conv_wide * padded[offset:offset + LENGTH], axis=0)) for offset in range(KERNEL)], axis=1)
        grad_pad = jnp.pad(conv_wide, ((HALF, HALF), (0, 0)))
        glu_grad = jnp.zeros((LENGTH, C), jnp.float32)
        for offset in range(KERNEL):
            glu_grad = glu_grad + depth_weight[:, offset] * grad_pad[2 * HALF - offset:2 * HALF - offset + LENGTH]
        glu_grad = glu_grad * frame_mask
        input_row = jnp.concatenate([glu_grad * gate_sigmoid, glu_grad * values * gate_sigmoid * (1.0 - gate_sigmoid)], axis=1)
        return (input_row.astype(jnp.bfloat16), depth_part)
    input_grad, depth_parts = lax.map(third, (glu_input, out_grad, lengths))
    depth_grad = grad_scale * lax.optimization_barrier(jnp.sum(depth_parts, axis=0))
    return (input_grad, proj_grad, depth_grad, grad_scale * gain_sum, grad_scale * shift_sum)
```

```python
import functools
import math

import jax
import jax.numpy as jnp
from jax import lax
from jax.experimental import pallas as pl
from jax.experimental.pallas import tpu as pltpu
from jax.sharding import Mesh
from jax.sharding import PartitionSpec as P

XY = ("seq_0", "seq_1")
SEQ = ("seq_0", "seq_1", "seq_2")
CORE_DP = ("seq_2", "dp")

EPSILON = 1e-05
TAPS = 31
HALF = 15
EDGE = 16
WIDE = 32
LANES = 128

F32 = jnp.float32
BF16 = jnp.bfloat16


def sigmoid(x):
    return 0.5 + 0.5 * jnp.tanh(0.5 * x)


def rows_per_step(rows):
    return max(r for r in range(8, 97, 8) if rows % r == 0)


def rows_iota(rows):
    return lax.broadcasted_iota(jnp.int32, (rows, LANES), 0)


def fold(x):
    return jnp.sum(x.reshape(x.shape[0] // 8, 8, LANES), axis=0)


def shifted_taps(read, rows, combine):
    for residue in range(8):
        block = read(residue, rows + 24)
        for step in range(4):
            k = 8 * step + residue - 1
            if 0 <= k < TAPS:
                combine(k, block[8 * step : 8 * step + rows])


def glu_kernel(meta, val, gate, low_val, low_gate, high_val, high_gate, taps, glu, conv, stats):
    frames = val.shape[0]
    first, length = meta[0], meta[1]

    def put(at, rows, v, g):
        pos = first - WIDE + at + rows_iota(rows)
        ok = (pos >= 0) & (pos < length)
        out = jnp.where(ok, v.astype(F32) * sigmoid(g.astype(F32)), 0.0)
        glu[pl.ds(at, rows), :] = out.astype(BF16).astype(F32)

    put(0, WIDE, low_val[0:WIDE, :], low_gate[0:WIDE, :])
    put(WIDE + frames, WIDE, high_val[0:WIDE, :], high_gate[0:WIDE, :])
    part = rows_per_step(frames)
    part = part if part % 16 == 0 else frames

    def put_own(i, _):
        at = pl.multiple_of(i * part, 16)
        put(WIDE + at, part, val[pl.ds(at, part), :], gate[pl.ds(at, part), :])
        return 0

    lax.fori_loop(0, frames // part, put_own, 0)

    total = frames + 2 * EDGE
    rows = rows_per_step(total)

    def step(i, carry):
        at = pl.multiple_of(i * rows, 8)
        acc = [jnp.zeros((rows, LANES), F32)]

        def add(k, window):
            acc[0] = acc[0] + taps[k : k + 1, :] * window

        shifted_taps(lambda s, n: glu[pl.ds(at + s, n), :], rows, add)
        conv[pl.ds(at, rows), :] = acc[0]
        idx = at + rows_iota(rows)
        own = (idx >= EDGE) & (idx < EDGE + frames) & (first - EDGE + idx < length)
        kept = jnp.where(own, acc[0], 0.0)
        return carry[0] + fold(kept), carry[1] + fold(kept * kept)

    zero = jnp.zeros((8, LANES), F32)
    s, q = lax.fori_loop(0, total // rows, step, (zero, zero))
    stats[0:1, :] = jnp.sum(s, axis=0, keepdims=True)
    stats[1:2, :] = jnp.sum(q, axis=0, keepdims=True)


def correlate(first, length, frames, source, glu, acc):
    rows = rows_per_step(frames)
    acc[...] = jnp.zeros_like(acc)

    def step(i, _):
        at = pl.multiple_of(i * rows, 8)
        ok = first + at + rows_iota(rows) < length
        mine = jnp.where(ok, source[pl.ds(EDGE + at, rows), :], 0.0)

        def add(k, window):
            acc[8 * k : 8 * k + 8, :] += fold(mine * window)

        shifted_taps(lambda s, n: glu[pl.ds(EDGE + at + s, n), :], rows, add)
        return 0

    lax.fori_loop(0, frames // rows, step, 0)


def spread(acc):
    return jnp.sum(acc[...].reshape(TAPS + 1, 8, LANES), axis=1)


def early_kernel(meta, glu, conv, out, acc):
    frames = conv.shape[0] - 2 * EDGE
    first, length = meta[0], meta[1]
    shape = (TAPS + 1, frames + 2 * WIDE)
    frame = (
        lax.broadcasted_iota(jnp.int32, shape, 1)
        - lax.broadcasted_iota(jnp.int32, shape, 0)
        - (EDGE + 1)
    )
    pick = (frame >= 0) & (frame < frames) & (first + frame < length)
    out[0] = jnp.dot(
        jnp.where(pick, 1.0, 0.0).astype(BF16), glu[...].astype(BF16), preferred_element_type=F32
    )
    correlate(first, length, frames, conv, glu, acc)
    out[1] = spread(acc)


def depth_kernel(meta, glu, pre_grad, out, acc):
    frames = pre_grad.shape[0] - 2 * EDGE
    correlate(meta[0], meta[1], frames, pre_grad, glu, acc)
    out[...] = spread(acc)


def act_grad_kernel(grad, low, high, weight, out):
    frames = grad.shape[0]
    side = jnp.concatenate([weight[z] for z in range(weight.shape[0])], axis=1)
    dims = (((1,), (1,)), ((), ()))
    edges = jnp.concatenate([low[WIDE : WIDE + EDGE, :], high[WIDE : WIDE + EDGE, :]], axis=0)
    both = lax.dot_general(edges, side, dims, preferred_element_type=F32)
    out[0:EDGE, :] = both[0:EDGE]
    out[EDGE + frames :, :] = both[EDGE:]
    out[EDGE : EDGE + frames, :] = lax.dot_general(grad[...], side, dims, preferred_element_type=F32)


def moments(stats, count, tmp):
    j = pl.program_id(0)
    tmp[...] = jnp.sum(stats[...], axis=0)
    mean = tmp[pl.ds(j, 1), :] / count
    var = tmp[pl.ds(j + 4, 1), :] / count - mean * mean
    return mean, lax.rsqrt(var + EPSILON)


def pre_kernel(meta, stats, count, gain, shift, conv, act_grad, act, pre_grad, sums, tmp):
    frames = conv.shape[0] - 2 * EDGE
    total = frames + 2 * EDGE
    first, length = meta[0], meta[1]
    mean, inv = moments(stats, count[0:1, :], tmp)
    g, b = gain[...], shift[...]

    def piece(at, rows, keep_act):
        normed = (conv[pl.ds(at, rows), :] - mean) * inv
        pre = g * normed + b
        sig = sigmoid(pre)
        pos = first - EDGE + at + rows_iota(rows)
        ok = (pos >= 0) & (pos < length)
        gone = jnp.where(ok, act_grad[pl.ds(at, rows), :] * sig * (1.0 + pre * (1.0 - sig)), 0.0)
        pre_grad[pl.ds(at, rows), :] = gone
        if keep_act:
            act[pl.ds(at - EDGE, rows), :] = jnp.where(ok, pre * sig, 0.0).astype(BF16)
        return gone, gone * normed

    piece(0, EDGE, False)
    piece(EDGE + frames, EDGE, False)
    rows = rows_per_step(frames)
    rows = rows if rows % 16 == 0 else frames

    def step(i, carry):
        one, two = piece(pl.multiple_of(EDGE + i * rows, 16), rows, True)
        return carry[0] + fold(two), carry[1] + fold(one)

    zero = jnp.zeros((8, LANES), F32)
    gs, ss = lax.fori_loop(0, frames // rows, step, (zero, zero))
    sums[0:1, :] = jnp.sum(gs, axis=0, keepdims=True)
    sums[1:2, :] = jnp.sum(ss, axis=0, keepdims=True)


def last_kernel(
    meta, stats, count, gain, sums, taps, conv, pre_grad, val, gate, out_val, out_gate, cg, tmp
):
    frames = val.shape[0]
    total = frames + 2 * EDGE
    first, length = meta[0], meta[1]
    n = count[0:1, :]
    mean, inv = moments(stats, n, tmp)
    scale = inv * gain[...]
    gm, sm = sums[0:1, :] / n, sums[1:2, :] / n
    rows = rows_per_step(total)

    def grad(i, _):
        at = pl.multiple_of(i * rows, 8)
        normed = (conv[pl.ds(at, rows), :] - mean) * inv
        pos = first - EDGE + at + rows_iota(rows)
        ok = (pos >= 0) & (pos < length)
        full = scale * (pre_grad[pl.ds(at, rows), :] - sm - normed * gm)
        cg[pl.ds(at, rows), :] = jnp.where(ok, full, 0.0).astype(BF16).astype(F32)
        return 0

    lax.fori_loop(0, total // rows, grad, 0)
    part = rows_per_step(frames)
    part = part if part % 16 == 0 else frames

    def step(i, _):
        at = pl.multiple_of(i * part, 16)
        acc = [jnp.zeros((part, LANES), F32)]

        def add(k, window):
            acc[0] = acc[0] + taps[TAPS - 1 - k : TAPS - k, :] * window

        shifted_taps(lambda s, m: cg[pl.ds(at + s, m), :], part, add)
        ok = first + at + rows_iota(part) < length
        gg = jnp.where(ok, acc[0], 0.0)
        sig = sigmoid(gate[pl.ds(at, part), :].astype(F32))
        v = val[pl.ds(at, part), :].astype(F32)
        through = gg * sig
        out_val[pl.ds(at, part), :] = through.astype(BF16)
        out_gate[pl.ds(at, part), :] = (through * v * (1.0 - sig)).astype(BF16)
        return 0

    lax.fori_loop(0, frames // part, step, 0)


def columns(rows, at=0):
    return pl.BlockSpec((rows, LANES), lambda j: (0, j + at))


def everything(shape):
    return pl.BlockSpec(shape, lambda j: (0,) * len(shape))


SCALARS = pl.BlockSpec(memory_space=pltpu.SMEM)


def call(kernel, name, blocks, ins, outs, out_shapes, scratch=(), flops=10**9, nbytes=4 * 10**6):
    return pl.pallas_call(
        kernel,
        grid=(blocks,),
        in_specs=ins,
        out_specs=outs,
        out_shape=out_shapes,
        scratch_shapes=list(scratch),
        name=name,
        cost_estimate=pl.CostEstimate(flops=flops, bytes_accessed=nbytes, transcendentals=0),
        compiler_params=pltpu.CompilerParams(dimension_semantics=("arbitrary",)),
    )


def to_everyone(array, axis):
    size = lax.axis_size(axis)
    return lax.all_to_all(
        jnp.broadcast_to(array[None], (size, *array.shape)), axis, 0, 0, tiled=True
    )


def split_high_low(x):
    high = lax.reduce_precision(x, 8, 7)
    return high.astype(BF16), (x - high).astype(BF16)


def on_device(glu_input, out_grad, lengths, depth_weight, bn_gain, bn_shift, proj_weight):
    _, frames, doubled = glu_input.shape
    channels = doubled // 2
    width = out_grad.shape[2]
    blocks = channels // LANES
    seq_count, dp_count = lax.axis_size(SEQ), lax.axis_size("dp")
    tiles = lax.axis_size(XY)
    own = channels // seq_count
    wide_own = width // dp_count
    scale = float(dp_count * frames * seq_count) ** (-0.5)
    core = lax.axis_index("seq_2")
    first = lax.axis_index(SEQ) * frames
    length = lax.dynamic_index_in_dim(lengths, lax.axis_index("dp"), 0, keepdims=False)
    meta = jnp.stack([first.astype(jnp.int32), length])
    count = jnp.broadcast_to(jnp.sum(lengths).astype(F32), (8, LANES))
    x, grad = glu_input[0], out_grad[0]
    taps = jnp.pad(depth_weight.T, ((0, 1), (0, 0)))
    gain, shift = bn_gain.reshape(1, channels), bn_shift.reshape(1, channels)
    ext, conv_rows = frames + 2 * WIDE, frames + 2 * EDGE

    forward = [(i, i + 1) for i in range(seq_count - 1)]
    backward = [(j, i) for i, j in forward]
    low = lax.ppermute(jnp.concatenate([x[-WIDE:], grad[-EDGE:]], axis=0), SEQ, forward)
    high = lax.ppermute(jnp.concatenate([x[:WIDE], grad[:EDGE]], axis=0), SEQ, backward)

    weight = to_everyone(proj_weight, SEQ).reshape(channels, wide_own)
    weight = to_everyone(weight, "dp")

    glu, conv, stats = call(
        glu_kernel,
        "glu_conv",
        blocks,
        [SCALARS, columns(frames), columns(frames, blocks)]
        + [columns(WIDE + EDGE), columns(WIDE + EDGE, blocks)] * 2
        + [columns(TAPS + 1)],
        [columns(ext), columns(conv_rows), columns(2)],
        [
            jax.ShapeDtypeStruct((ext, channels), F32),
            jax.ShapeDtypeStruct((conv_rows, channels), F32),
            jax.ShapeDtypeStruct((2, channels), F32),
        ],
    )(meta, x, x, low, low, high, high, taps)

    stats = to_everyone(stats.reshape(2 * blocks, LANES), XY).sum(axis=0)
    stats = to_everyone(stats, CORE_DP)
    all_stats = everything(stats.shape)

    early = call(
        early_kernel,
        "early_terms",
        blocks,
        [SCALARS, columns(ext), columns(conv_rows)],
        pl.BlockSpec((2, TAPS + 1, LANES), lambda j: (0, 0, j)),
        jax.ShapeDtypeStruct((2, TAPS + 1, channels), F32),
        [pltpu.VMEM((8 * (TAPS + 1), LANES), F32)],
    )(meta, glu, conv)

    act_grad = call(
        act_grad_kernel,
        "act_grad",
        channels // 256,
        [
            everything((frames, width)),
            everything((WIDE + EDGE, width)),
            everything((WIDE + EDGE, width)),
            pl.BlockSpec((dp_count, 256, wide_own), lambda j: (0, j, 0)),
        ],
        pl.BlockSpec((conv_rows, 256), lambda j: (0, j)),
        jax.ShapeDtypeStruct((conv_rows, channels), F32),
    )(grad, low, high, weight)

    act, pre_grad, sums = call(
        pre_kernel,
        "pre_grad",
        blocks,
        [SCALARS, all_stats, everything((8, LANES)), columns(1), columns(1)]
        + [columns(conv_rows)] * 2,
        [columns(frames), columns(conv_rows), columns(2)],
        [
            jax.ShapeDtypeStruct((frames, channels), BF16),
            jax.ShapeDtypeStruct((conv_rows, channels), F32),
            jax.ShapeDtypeStruct((2, channels), F32),
        ],
        [pltpu.VMEM((2 * blocks, LANES), F32)],
    )(meta, stats, count, gain, shift, conv, act_grad)

    terms = jnp.einsum("tc,td->cd", act, grad, preferred_element_type=F32)
    terms = terms.reshape(tiles, 2, own, width)
    theirs = lax.dynamic_index_in_dim(terms, 1 - core, 1, keepdims=False).astype(BF16)
    theirs = lax.ppermute(theirs, "seq_2", [(0, 1), (1, 0)])
    mine = lax.dynamic_index_in_dim(terms, core, 1, keepdims=False)

    late = call(
        depth_kernel,
        "depth_terms",
        blocks,
        [SCALARS, columns(ext), columns(conv_rows)],
        columns(TAPS + 1),
        jax.ShapeDtypeStruct((TAPS + 1, channels), F32),
        [pltpu.VMEM((8 * (TAPS + 1), LANES), F32)],
    )(meta, glu, pre_grad)

    depth = jnp.concatenate([early, late[None]], axis=0).reshape(3, TAPS + 1, tiles, 2 * own)
    depth = depth.transpose(2, 0, 1, 3).reshape(tiles, -1)
    depth_size = depth.shape[1]
    small = jnp.concatenate([depth, jnp.broadcast_to(sums.reshape(1, -1), (tiles, 2 * channels))], 1)
    small_size = small.shape[1]
    both = jnp.concatenate(split_high_low(small), axis=1)
    room = -(-both.shape[1] // (own * LANES)) * LANES
    both = jnp.pad(both, ((0, 0), (0, own * room - both.shape[1]))).reshape(tiles, own, room)
    message = jnp.concatenate([(mine + theirs.astype(F32)).astype(BF16), both], axis=2)
    message = lax.all_to_all(message, XY, 0, 0, tiled=True).astype(F32).sum(axis=0)
    proj = message[:, :width]
    both = message[:, width:].reshape(-1)
    small = both[:small_size] + both[small_size : 2 * small_size]

    here = (jnp.arange(2) == core)[:, None, None, None]
    proj = proj.reshape(1, own, dp_count, wide_own).transpose(0, 2, 1, 3)
    proj = jnp.where(here, proj, 0.0).reshape(2 * dp_count, -1)
    depth = small[:depth_size].reshape(3 * (TAPS + 1), 2, own).transpose(1, 0, 2).reshape(2, 1, -1)
    depth = jnp.broadcast_to(depth, (2, dp_count, depth.shape[2])).reshape(2 * dp_count, -1)
    sums = jnp.broadcast_to(small[depth_size:][None], (2 * dp_count, 2 * channels))
    message = jnp.concatenate([proj, depth, sums], axis=1)
    size = message.shape[1]
    room = -(-size // 1024) * 1024
    message = jnp.pad(message, ((0, 0), (0, room - size))).reshape(2 * dp_count, room // LANES, LANES)
    message = lax.all_to_all(message, CORE_DP, 0, 0, tiled=True).sum(axis=0).reshape(-1)
    at = own * wide_own
    proj_grad = message[:at].reshape(own, wide_own) * scale
    depth = message[at : at + 3 * (TAPS + 1) * own].reshape(3, TAPS + 1, own)
    at += 3 * (TAPS + 1) * own
    sums = message[at : at + 2 * channels].reshape(2, channels)

    out_val, out_gate = call(
        last_kernel,
        "input_grad",
        blocks,
        [SCALARS, all_stats, everything((8, LANES)), columns(1), columns(2), columns(TAPS + 1)]
        + [columns(conv_rows)] * 2
        + [columns(frames), columns(frames, blocks)],
        [columns(frames)] * 2,
        [jax.ShapeDtypeStruct((frames, channels), BF16)] * 2,
        [pltpu.VMEM((conv_rows, LANES), F32), pltpu.VMEM((2 * blocks, LANES), F32)],
    )(meta, stats, count, gain, sums, taps, conv, pre_grad, x, x)
    input_grad = jnp.concatenate([out_val, out_gate], axis=1)[None]

    begin = lax.axis_index(SEQ) * own
    n = count[0, 0]
    total = stats.sum(axis=0).reshape(2, channels)
    total = lax.dynamic_slice_in_dim(total, begin, own, 1)
    mean = total[0] / n
    inv = lax.rsqrt(total[1] / n - mean * mean + EPSILON)
    sums = lax.dynamic_slice_in_dim(sums, begin, own, 1)
    own_gain = lax.dynamic_slice_in_dim(bn_gain, begin, own)
    flat, with_conv, with_grad = depth[0], depth[1], depth[2]
    depth_grad = with_grad - sums[1] / n * flat - sums[0] / n * inv * (with_conv - mean * flat)
    depth_grad = (depth_grad * (scale * inv * own_gain)).T[:, :TAPS]
    return (input_grad, proj_grad, depth_grad, sums[0] * scale, sums[1] * scale)


def solution(mesh):
    seq, dp = mesh.shape["seq"], mesh.shape["dp"]
    x = 4 if seq >= 64 else 2
    finer = Mesh(
        mesh.devices.reshape(x, seq // (2 * x), 2, dp), ("seq_0", "seq_1", "seq_2", "dp")
    )
    return jax.shard_map(
        on_device,
        mesh=finer,
        in_specs=(P("dp", SEQ, None), P("dp", SEQ, None), P(), P(), P(), P(), P(SEQ, "dp")),
        out_specs=(P("dp", SEQ, None), P(SEQ, "dp"), P(SEQ, None), P(SEQ), P(SEQ)),
        check_vma=False,
    )
```
